8 devices in a mesh: dp: 2 (over z, y), tp: 4 (over x, core).
Axes of the slice: x: 2, y: 2, z: 1, core: 2. Of those that a mesh axis runs over, the one named last changes fastest.
Arguments:
- x_in: bfloat16 [16, 2048, 1024], P('dp', 'tp'), parts along dimension 0
- ln_gain: float32 [2, 1024], replicated
- ln_bias: float32 [2, 1024], replicated
- w_qkv: bfloat16 [2, 1024, 3, 16, 64], P(None, None, None, 'tp')
- w_out: bfloat16 [2, 16, 64, 1024], P(None, 'tp')
- b_out: float32 [2, 1024], replicated
- w_up: bfloat16 [2, 1024, 4096], P(None, None, 'tp')
- b_up: float32 [2, 4096], P(None, 'tp')
- w_down: bfloat16 [2, 4096, 1024], P(None, 'tp')
- b_down: float32 [2, 1024], replicated
Outputs:
- output: bfloat16 [16, 2048, 1024], P('dp', 'tp'), parts along dimension 0
There are 2 independent parts. The reference program is written for one: setup_inputs(seed, part) draws one part's arguments, and reference() takes and returns one part's arrays. A program takes and returns all parts, laid end to end along the dimension named above; an argument that names none is the same for every part.
All inputs are finite; a program needn't handle non-finite values.
Results may differ from the reference program's by a relative error of at most 0.0128649.
Values are sent between devices in bfloat16 or wider.
A program may use at most 1 GiB of HBM per device.

```python
import math
import jax
import jax.numpy as jnp
from jax import lax

BATCH_SIZE = 8
SEQ_LEN = 2048
MODEL_DIM = 1024
N_HEADS = 16
HEAD_DIM = 64
FFN_WIDTH = 4096
NUM_LAYERS = 2
LN_EPS = 1e-5


def setup_inputs(seed: int = 0, part: int = 0) -> dict:
    key = jax.random.key(seed)
    shared = jax.random.split(key, 9)
    part_keys = jax.random.split(jax.random.fold_in(key, part), 2)
    tok_scale = 0.5 + jax.random.uniform(part_keys[0], (BATCH_SIZE, SEQ_LEN, 1), jnp.float32)
    x_in = jax.random.normal(part_keys[1], (BATCH_SIZE, SEQ_LEN, MODEL_DIM), jnp.float32) * tok_scale
    logit_std = math.sqrt(max(math.log(SEQ_LEN / 32.0), 1.0))
    qk_gain = math.sqrt(logit_std)
    comp_gain = jnp.array([qk_gain, qk_gain, 1.0], jnp.float32).reshape(1, 1, 3, 1, 1)
    in_scale = MODEL_DIM ** -0.5
    w_qkv = jax.random.normal(shared[0], (NUM_LAYERS, MODEL_DIM, 3, N_HEADS, HEAD_DIM), jnp.float32) * (in_scale * comp_gain)
    w_out = jax.random.normal(shared[1], (NUM_LAYERS, N_HEADS, HEAD_DIM, MODEL_DIM), jnp.float32) * (1.5 * in_scale)
    w_up = jax.random.normal(shared[2], (NUM_LAYERS, MODEL_DIM, FFN_WIDTH), jnp.float32) * in_scale
    w_down = jax.random.normal(shared[3], (NUM_LAYERS, FFN_WIDTH, MODEL_DIM), jnp.float32) * FFN_WIDTH ** -0.5
    ln_gain = 1.0 + 0.2 * jax.random.normal(shared[4], (NUM_LAYERS, MODEL_DIM), jnp.float32)
    ln_bias = 0.2 * jax.random.normal(shared[5], (NUM_LAYERS, MODEL_DIM), jnp.float32)
    b_out = 0.1 * jax.random.normal(shared[6], (NUM_LAYERS, MODEL_DIM), jnp.float32)
    b_up = 0.3 * jax.random.normal(shared[7], (NUM_LAYERS, FFN_WIDTH), jnp.float32)
    b_down = 0.1 * jax.random.normal(shared[8], (NUM_LAYERS, MODEL_DIM), jnp.float32)
    return {
        'x_in': x_in.astype(jnp.bfloat16),
        'ln_gain': ln_gain,
        'ln_bias': ln_bias,
        'w_qkv': w_qkv.astype(jnp.bfloat16),
        'w_out': w_out.astype(jnp.bfloat16),
        'b_out': b_out,
        'w_up': w_up.astype(jnp.bfloat16),
        'b_up': b_up,
        'w_down': w_down.astype(jnp.bfloat16),
        'b_down': b_down,
    }


def layer_norm(residual, gain, bias):
    row_mean = jnp.mean(residual, axis=-1, keepdims=True)
    centered = residual - row_mean
    row_var = jnp.mean(centered * centered, axis=-1, keepdims=True)
    return (centered * lax.rsqrt(row_var + LN_EPS) * gain + bias).astype(jnp.bfloat16)


def query_block(batch, heads, q_len, k_len):
    block = q_len
    while block % 2 == 0 and block > 16 and batch * heads * block * k_len > 2 ** 24:
        block = block // 2
    return block


def causal_attention(queries, keys, values):
    batch, seq_len, heads, head_dim = queries.shape
    block = query_block(batch, heads, seq_len, seq_len)
    inv_sqrt = head_dim ** -0.5
    key_pos = jnp.arange(seq_len)
    keys_f = keys.astype(jnp.float32)
    values_f = values.astype(jnp.float32)

    def one_block(index):
        q_blk = lax.dynamic_slice_in_dim(queries, index * block, block, axis=1).astype(jnp.float32)
        scores = jnp.einsum('bqhe,bkhe->bhqk', q_blk, keys_f) * inv_sqrt
        q_pos = index * block + jnp.arange(block)
        scores = jnp.where(key_pos[None, :] <= q_pos[:, None], scores, -jnp.inf)
        attn_prob = jax.nn.softmax(scores, axis=-1).astype(jnp.bfloat16).astype(jnp.float32)
        return jnp.einsum('bhqk,bkhe->bqhe', attn_prob, values_f).astype(jnp.bfloat16)

    out_blocks = lax.map(one_block, jnp.arange(seq_len // block))
    return jnp.moveaxis(out_blocks, 0, 1).reshape(batch, seq_len, heads, head_dim)


def one_layer(residual, params):
    ln_gain, ln_bias, w_qkv, w_out, b_out, w_up, b_up, w_down, b_down = params
    normed = layer_norm(residual, ln_gain, ln_bias)
    normed_f = normed.astype(jnp.float32)
    qkv_all = jnp.einsum('bsd,dthe->bsthe', normed_f, w_qkv.astype(jnp.float32)).astype(jnp.bfloat16)
    attn_out = causal_attention(qkv_all[:, :, 0], qkv_all[:, :, 1], qkv_all[:, :, 2])
    attn_sum = jnp.einsum('bshe,hed->bsd', attn_out.astype(jnp.float32), w_out.astype(jnp.float32))
    hidden = jnp.einsum('bsd,df->bsf', normed_f, w_up.astype(jnp.float32)) + b_up
    gelu_out = jax.nn.gelu(hidden, approximate=True).astype(jnp.bfloat16)
    mlp_sum = jnp.einsum('bsf,fd->bsd', gelu_out.astype(jnp.float32), w_down.astype(jnp.float32))
    return residual + (attn_sum + mlp_sum + b_out + b_down), None


def reference(x_in, ln_gain, ln_bias, w_qkv, w_out, b_out, w_up, b_up, w_down, b_down):
    residual = x_in.astype(jnp.float32)
    residual, _ = lax.scan(one_layer, residual, (ln_gain, ln_bias, w_qkv, w_out, b_out, w_up, b_up, w_down, b_down))
    return residual.astype(jnp.bfloat16)
```

```python
import functools
import math

import jax
import jax.numpy as jnp
from jax import lax
from jax.experimental import pallas as pl
from jax.experimental.pallas import tpu as pltpu
from jax.sharding import PartitionSpec as P


LN_EPS = 1e-5
BLOCK_TOKENS = 512
TP_SIZE = 4
BLOCK_Q = 256
BLOCK_K = 256
VMEM_LIMIT = 58 * 1024 * 1024
SQRT_2_OVER_PI = math.sqrt(2.0 / math.pi)
LOG2_E = math.log2(math.e)


def layer_norm(residual, gain, bias):
    row_mean = jnp.mean(residual, axis=-1, keepdims=True)
    centered = residual - row_mean
    row_var = jnp.mean(centered * centered, axis=-1, keepdims=True)
    return (centered * lax.rsqrt(row_var + LN_EPS) * gain + bias).astype(jnp.bfloat16)


def gelu_tanh(x):
    inner = x * (SQRT_2_OVER_PI + (SQRT_2_OVER_PI * 0.044715) * (x * x))
    half = 0.5 * x
    return half + half * jnp.tanh(inner)


def dot(a, b):
    return lax.dot_general(a, b, (((1,), (0,)), ((), ())), preferred_element_type=jnp.float32)


def cost(flops, nbytes):
    return pl.CostEstimate(flops=flops, transcendentals=0, bytes_accessed=nbytes)


def start_qkv_copies(w_hbm, w_vmem, sem):
    parts, rows, _ = w_hbm.shape
    chunks = w_vmem.shape[0]
    for i in range(parts):
        half, chunk = divmod(i, chunks)
        pltpu.make_async_copy(w_hbm.at[i], w_vmem.at[chunk, pl.ds(half * rows, rows)], sem).start()


def wait_qkv_copies(w_hbm, w_vmem, sem):
    parts, rows, _ = w_hbm.shape
    chunks = w_vmem.shape[0]
    for i in range(parts):
        half, chunk = divmod(i, chunks)
        pltpu.make_async_copy(w_hbm.at[i], w_vmem.at[chunk, pl.ds(half * rows, rows)], sem).wait()


def project_qkv(h, w_vmem, qkv_ref):
    for c in range(w_vmem.shape[0]):
        qkv_ref[c] = dot(h, w_vmem[c]).astype(jnp.bfloat16)


def qkv_kernel(x_ref, gain_ref, bias_ref, w_hbm, qkv_ref, w_vmem, sem):
    first = pl.program_id(0) == 0

    @pl.when(first)
    def _():
        start_qkv_copies(w_hbm, w_vmem, sem)

    h = layer_norm(x_ref[...].astype(jnp.float32), gain_ref[...], bias_ref[...])

    @pl.when(first)
    def _():
        wait_qkv_copies(w_hbm, w_vmem, sem)

    project_qkv(h, w_vmem, qkv_ref)


def qkv_call(x, seq, tokens, gain, bias, w_qkv):
    width = x.shape[1]
    offset = seq * tokens // BLOCK_TOKENS
    parts, rows, cols = w_qkv.shape
    chunks = parts * rows // width
    return pl.pallas_call(
        qkv_kernel,
        grid=(tokens // BLOCK_TOKENS,),
        in_specs=[
            pl.BlockSpec((BLOCK_TOKENS, width), lambda i: (offset + i, 0)),
            pl.BlockSpec((1, width), lambda i: (0, 0)),
            pl.BlockSpec((1, width), lambda i: (0, 0)),
            pl.BlockSpec(memory_space=pl.ANY),
        ],
        out_specs=pl.BlockSpec((chunks, BLOCK_TOKENS, cols), lambda i: (0, i, 0)),
        out_shape=jax.ShapeDtypeStruct((chunks, tokens, cols), jnp.bfloat16),
        scratch_shapes=[pltpu.VMEM((chunks, width, cols), jnp.bfloat16), pltpu.SemaphoreType.DMA],
        compiler_params=pltpu.CompilerParams(
            dimension_semantics=('arbitrary',), vmem_limit_bytes=VMEM_LIMIT),
        cost_estimate=cost(2 * tokens * width * chunks * cols, 2 * tokens * (width + chunks * cols) + 2 * width * chunks * cols),
        name='ln_qkv',
    )(x, gain, bias, w_qkv)


def attention_kernel(*refs, head_dim):
    q_ref, k_ref, v_ref = refs[:3]
    o_ref, s_ref, vx_ref = refs[-3:]
    seq_len, pair = q_ref.shape[1:]
    vx_ref[:, :pair] = v_ref[0]
    vx_ref[:, pair:] = jnp.ones((seq_len, pair), jnp.bfloat16)
    low_lane = lax.broadcasted_iota(jnp.int32, (1, pair), 1) < head_dim
    q_pos = lax.broadcasted_iota(jnp.int32, (BLOCK_Q, BLOCK_K), 0)
    k_pos = lax.broadcasted_iota(jnp.int32, (BLOCK_Q, BLOCK_K), 1)
    causal = k_pos <= q_pos
    inv_sqrt = head_dim ** -0.5
    n_blocks = seq_len // BLOCK_Q
    units = [(block, head) for block in range(n_blocks) for head in range(2)]

    def head_query(unit):
        block, head = unit
        q_blk = q_ref[0, block * BLOCK_Q:(block + 1) * BLOCK_Q, :] * jnp.bfloat16(inv_sqrt)
        keep = low_lane if head == 0 else jnp.logical_not(low_lane)
        return jnp.where(keep, q_blk, jnp.zeros_like(q_blk))

    def score_chunk(unit_idx, q_h, c, run_max):
        block, _ = units[unit_idx]
        k_blk = k_ref[0, c * BLOCK_K:(c + 1) * BLOCK_K, :]
        s = lax.dot_general(q_h, k_blk, (((1,), (1,)), ((), ())), preferred_element_type=jnp.float32)
        if c == block:
            s = jnp.where(causal, s, -jnp.inf)
        s_ref[unit_idx % 2, :, c * BLOCK_K:(c + 1) * BLOCK_K] = s
        chunk_max = s[:, :128]
        for j in range(1, BLOCK_K // 128):
            chunk_max = jnp.maximum(chunk_max, s[:, j * 128:(j + 1) * 128])
        return chunk_max if run_max is None else jnp.maximum(run_max, chunk_max)

    def value_chunk(unit_idx, row_max, c):
        s = s_ref[unit_idx % 2, :, c * BLOCK_K:(c + 1) * BLOCK_K]
        p = jnp.exp2((s - row_max) * LOG2_E).astype(jnp.bfloat16)
        return dot(p, vx_ref[c * BLOCK_K:(c + 1) * BLOCK_K, :])

    run_max = None
    row_max = None
    held = None
    for step in range(len(units) + 1):
        n_score = units[step][0] + 1 if step < len(units) else 0
        n_value = units[step - 1][0] + 1 if step > 0 else 0
        if step > 0:
            row_max = jnp.max(run_max, axis=1, keepdims=True)
        run_max = None
        acc = None
        q_h = head_query(units[step]) if n_score else None
        for c in range(max(n_score, n_value)):
            if c < n_score:
                run_max = score_chunk(step, q_h, c, run_max)
            if c < n_value:
                part = value_chunk(step - 1, row_max, c)
                acc = part if acc is None else acc + part
        if n_value:
            block, head = units[step - 1]
            out = acc[:, :pair] / acc[:, pair:]
            if head == 0:
                held = out
            else:
                o_ref[block * BLOCK_Q:(block + 1) * BLOCK_Q, :] = jnp.where(low_lane, held, out).astype(jnp.bfloat16)


def attention_call(qkv, qkv_seq, seq, batch, seq_len, head_dim, buffer):
    chunks, _, cols = qkv.shape
    pair = 2 * head_dim
    subs = cols // 3 // pair
    spec = lambda t: pl.BlockSpec((1, seq_len, pair), lambda g: (g // subs, qkv_seq, t * subs + g % subs))
    held = [] if buffer is None else [buffer]
    return pl.pallas_call(
        functools.partial(attention_kernel, head_dim=head_dim),
        grid=(chunks * subs,),
        in_specs=[spec(0), spec(1), spec(2)] + [pl.BlockSpec(memory_space=pl.ANY) for _ in held],
        out_specs=pl.BlockSpec((seq_len, pair), lambda g: (seq, g)),
        out_shape=jax.ShapeDtypeStruct((batch * seq_len, chunks * subs * pair), jnp.bfloat16),
        input_output_aliases={3: 0} if held else {},
        scratch_shapes=[pltpu.VMEM((2, BLOCK_Q, seq_len), jnp.float32), pltpu.VMEM((seq_len, 2 * pair), jnp.bfloat16)],
        compiler_params=pltpu.CompilerParams(
            dimension_semantics=('arbitrary',), vmem_limit_bytes=VMEM_LIMIT),
        cost_estimate=cost(9 * seq_len * seq_len * chunks * cols // 4, 2 * seq_len * chunks * (cols + subs * pair)),
        name='causal_attention',
    )(qkv, qkv, qkv, *held)


def ffn_body(first, r_ref, o_ref, gain_ref, bias_ref, bsum_ref, bup_ref, wout_hbm, wup_hbm, wdown_hbm,
             acc_ref, wout_vmem, wup_vmem, wdown_vmem, sems):
    parts = wup_vmem.shape[0]
    early = 2
    out_rows = wout_hbm.shape[1]
    early_copies = []
    for i in range(parts):
        pos = (i % TP_SIZE) * (parts // TP_SIZE) + i // TP_SIZE
        early_copies.append(pltpu.make_async_copy(wout_hbm.at[i], wout_vmem.at[pl.ds(pos * out_rows, out_rows)], sems.at[0]))
    late_copies = []
    for lo, hi, sem, group in ((0, early, 0, early_copies), (early, parts, 1, late_copies)):
        for src, dst in ((wup_hbm, wup_vmem), (wdown_hbm, wdown_vmem)):
            group.append(pltpu.make_async_copy(src.at[pl.ds(lo, hi - lo)], dst.at[pl.ds(lo, hi - lo)], sems.at[sem]))

    @pl.when(first)
    def _():
        for cp in early_copies + late_copies:
            cp.start()

    h = layer_norm(r_ref[...].astype(jnp.float32), gain_ref[...], bias_ref[...])

    def wait_all(copies):
        @pl.when(first)
        def _():
            for cp in copies:
                cp.wait()

    wait_all(early_copies)
    acc_ref[...] = dot(o_ref[...], wout_vmem[...]) + bsum_ref[...]
    hidden = dot(h, wup_vmem[0]) + bup_ref[0]
    for c in range(parts):
        if c + 1 == early:
            wait_all(late_copies)
        ahead = dot(h, wup_vmem[c + 1]) + bup_ref[c + 1] if c + 1 < parts else None
        gelu_out = gelu_tanh(hidden).astype(jnp.bfloat16)
        acc_ref[...] += dot(gelu_out, wdown_vmem[c])
        hidden = ahead
    return r_ref[...].astype(jnp.float32) + acc_ref[...]


def mid_kernel(r_ref, o_ref, gain_ref, bias_ref, bsum_ref, bup_ref, ngain_ref, nbias_ref, wout_hbm, wup_hbm, wdown_hbm,
               wqkv_hbm, res_ref, qkv_ref, acc_ref, wout_vmem, wup_vmem, wdown_vmem, wqkv_vmem, sems):
    first = pl.program_id(0) == 0

    @pl.when(first)
    def _():
        start_qkv_copies(wqkv_hbm, wqkv_vmem, sems.at[2])

    r_new = ffn_body(first, r_ref, o_ref, gain_ref, bias_ref, bsum_ref, bup_ref, wout_hbm, wup_hbm, wdown_hbm,
                     acc_ref, wout_vmem, wup_vmem, wdown_vmem, sems)
    res_ref[...] = r_new
    h_next = layer_norm(r_new, ngain_ref[...], nbias_ref[...])

    @pl.when(first)
    def _():
        wait_qkv_copies(wqkv_hbm, wqkv_vmem, sems.at[2])

    project_qkv(h_next, wqkv_vmem, qkv_ref)


def last_kernel(rows_ref, r_ref, o_ref, gain_ref, bias_ref, bsum_ref, bup_ref, wout_hbm, wup_hbm, wdown_hbm,
                y_ref, acc_ref, wout_vmem, wup_vmem, wdown_vmem, sems):
    first = pl.program_id(0) == 0
    y_ref[...] = ffn_body(first, r_ref, o_ref, gain_ref, bias_ref, bsum_ref, bup_ref, wout_hbm, wup_hbm, wdown_hbm,
                          acc_ref, wout_vmem, wup_vmem, wdown_vmem, sems).astype(jnp.bfloat16)


def mid_call(r, o, gain, bias, bsum, bup, ngain, nbias, w_out, w_up, w_down, w_qkv):
    tokens, width = r.shape
    parts, rows, cols = w_qkv.shape
    chunks = parts * rows // width
    row = pl.BlockSpec((BLOCK_TOKENS, width), lambda i: (i, 0))
    vec = pl.BlockSpec((1, width), lambda i: (0, 0))
    bup_spec = pl.BlockSpec(bup.shape, lambda i: (0, 0, 0))
    hbm = pl.BlockSpec(memory_space=pl.ANY)
    return pl.pallas_call(
        mid_kernel,
        grid=(tokens // BLOCK_TOKENS,),
        in_specs=[row, row, vec, vec, vec, bup_spec, vec, vec, hbm, hbm, hbm, hbm],
        out_specs=[row, pl.BlockSpec((chunks, BLOCK_TOKENS, cols), lambda i: (0, i, 0))],
        out_shape=[jax.ShapeDtypeStruct((tokens, width), jnp.float32),
                   jax.ShapeDtypeStruct((chunks, tokens, cols), jnp.bfloat16)],
        scratch_shapes=[pltpu.VMEM((BLOCK_TOKENS, width), jnp.float32), pltpu.VMEM((width, width), jnp.bfloat16),
                        pltpu.VMEM(w_up.shape, jnp.bfloat16), pltpu.VMEM(w_down.shape, jnp.bfloat16),
                        pltpu.VMEM((chunks, width, cols), jnp.bfloat16), pltpu.SemaphoreType.DMA((3,))],
        compiler_params=pltpu.CompilerParams(
            dimension_semantics=('arbitrary',), vmem_limit_bytes=VMEM_LIMIT),
        cost_estimate=cost(24 * tokens * width * width, 20 * tokens * width),
        name='ffn_qkv',
    )(r, o, gain, bias, bsum, bup, ngain, nbias, w_out, w_up, w_down, w_qkv)


def last_call(r, o, gain, bias, bsum, bup, w_out, w_up, w_down, start, blocks, blk):
    width = r.shape[1]
    count = blocks.shape[0] * blk
    per = blk // BLOCK_TOKENS
    offset = start // BLOCK_TOKENS
    row = pl.BlockSpec((BLOCK_TOKENS, width), lambda i, rows: (offset + rows[i // per] * per + i % per, 0))
    vec = pl.BlockSpec((1, width), lambda i, rows: (0, 0))
    hbm = pl.BlockSpec(memory_space=pl.ANY)
    return pl.pallas_call(
        last_kernel,
        grid_spec=pltpu.PrefetchScalarGridSpec(
            num_scalar_prefetch=1,
            grid=(count // BLOCK_TOKENS,),
            in_specs=[row, pl.BlockSpec((BLOCK_TOKENS, width), lambda i, rows: (rows[i // per] * per + i % per, 0)),
                      vec, vec, vec, pl.BlockSpec(bup.shape, lambda i, rows: (0, 0, 0)), hbm, hbm, hbm],
            out_specs=pl.BlockSpec((BLOCK_TOKENS, width), lambda i, rows: (i, 0)),
            scratch_shapes=[pltpu.VMEM((BLOCK_TOKENS, width), jnp.float32), pltpu.VMEM((width, width), jnp.bfloat16),
                            pltpu.VMEM(w_up.shape, jnp.bfloat16), pltpu.VMEM(w_down.shape, jnp.bfloat16),
                            pltpu.SemaphoreType.DMA((2,))]),
        out_shape=jax.ShapeDtypeStruct((count, width), jnp.bfloat16),
        compiler_params=pltpu.CompilerParams(
            dimension_semantics=('arbitrary',), vmem_limit_bytes=VMEM_LIMIT),
        cost_estimate=cost(18 * count * width * width, 8 * count * width),
        name='ffn_out',
    )(blocks, r, o, gain, bias, bsum, bup, w_out, w_up, w_down)


def solution(mesh):
    tp_size = mesh.shape['tp']
    dp_size = mesh.shape['dp']
    act_spec = P('dp', 'tp', None)

    def local_fn(x_in, ln_gain, ln_bias, w_qkv, w_out, b_out, w_up, b_up, w_down, b_down):
        n_layers, width, _, heads, head_dim = w_qkv.shape
        dp_idx = lax.axis_index('dp')
        tp_idx = lax.axis_index('tp')
        batch_all, blk, _ = x_in.shape
        batch = batch_all // tp_size
        seq_len = blk * tp_size
        tokens = batch * seq_len

        def gather(shard):
            return lax.all_gather(shard, ('dp', 'tp'), axis=0, tiled=False)

        def half(arr, axis):
            size = arr.shape[axis] // dp_size
            return lax.dynamic_slice_in_dim(arr, dp_idx * size, size, axis)

        def qkv_shard(layer):
            return half(w_qkv[layer].reshape(width, 3 * heads * head_dim), 0)

        def ffn_shards(layer):
            return half(w_out[layer].reshape(heads * head_dim, width), 0), half(w_up[layer], 1), half(w_down[layer], 0)

        def exchange(pieces):
            return [piece if k == 0 else lax.ppermute(piece, 'tp', [(i, i ^ k) for i in range(tp_size)])
                    for k, piece in pieces]

        def ffn_weights(shards):
            return tuple(gather(shard) for shard in shards)

        bup_all = lax.all_gather(half(b_up, 1), ('dp', 'tp'), axis=1, tiled=False)
        bsum = b_out + b_down
        peers = [jnp.bitwise_xor(tp_idx, k) for k in range(tp_size)]
        far_first = [k for k in reversed(range(tp_size))]

        x_parts = x_in.reshape(tp_size, batch, blk, width)
        x_send = [[lax.dynamic_slice(x_parts, (peers[k], b, 0, 0), (1, 1, blk, width)) for k in far_first]
                  for b in range(batch)]
        x_all = jnp.zeros((batch, tp_size, blk, width), jnp.bfloat16)

        def place(x_all, b, received):
            for k, piece in zip(far_first, received):
                x_all = lax.dynamic_update_slice(x_all, piece, (b, peers[k], 0, 0))
            return x_all

        received = exchange(list(zip(far_first, x_send[0])))
        first_shard = qkv_shard(0)
        qkv_w = gather(first_shard)
        _, received = lax.optimization_barrier((first_shard, received))
        x_all = place(x_all, 0, received)
        x_all, x_send[1:], shards = lax.optimization_barrier((x_all, x_send[1:], ffn_shards(0)))
        received = [exchange(list(zip(far_first, send))) for send in x_send[1:]]
        weights = [ffn_weights(shards)]

        def norm_args(layer):
            return ln_gain[layer:layer + 1], ln_bias[layer:layer + 1]

        later = [(qkv_shard(layer), ffn_shards(layer)) for layer in range(1, n_layers)]
        qkv = [qkv_call(x_all.reshape(tokens, width), 0, seq_len, *norm_args(0), qkv_w)]
        attn = attention_call(qkv[0], 0, 0, batch, seq_len, head_dim, None)
        for b in range(1, batch):
            x_all, got, attn, later = lax.optimization_barrier((x_all, received[b - 1], attn, later))
            x_all = place(x_all, b, got)
            qkv.append(qkv_call(x_all.reshape(tokens, width), b, seq_len, *norm_args(0), qkv_w))
            attn = attention_call(qkv[b], 0, b, batch, seq_len, head_dim, attn)
        later_qkv = []
        for layer, (qkv_part, ffn_part) in enumerate(later):
            later_qkv.append(gather(qkv_part))
            weights.append(ffn_weights(ffn_part))

        def args(layer):
            return (*norm_args(layer), bsum[layer:layer + 1], bup_all[layer][:, None, :])

        residual = x_all.reshape(tokens, width)
        for layer in range(n_layers - 1):
            if layer:
                attn = None
                for b in range(batch):
                    attn = attention_call(qkv_all, b, b, batch, seq_len, head_dim, attn)
            residual, qkv_all = mid_call(residual, attn, *args(layer), *norm_args(layer + 1), *weights[layer],
                                         later_qkv[layer])
        layer = n_layers - 1
        y_out = jnp.zeros((tp_size, batch, blk, width), jnp.bfloat16)
        sent = []
        done = None
        for b in range(batch):
            if done is not None:
                qkv_all, done = lax.optimization_barrier((qkv_all, done))
            attn = attention_call(qkv_all, b, 0, 1, seq_len, head_dim, None)
            groups = [far_first] if b + 1 < batch else [far_first[:tp_size // 2], far_first[tp_size // 2:]]
            done = None
            for group in groups:
                order = jnp.stack([peers[k] for k in group]).astype(jnp.int32)
                if done is not None:
                    order, done = lax.optimization_barrier((order, done))
                    sent[-1] = (sent[-1][0], done, sent[-1][2])
                done = last_call(residual, attn, *args(layer), *weights[layer], b * seq_len, order, blk)
                sent.append((b, done, group))
        for b, y, group in sent:
            y = y.reshape(len(group), 1, 1, blk, width)
            for k, piece in zip(group, exchange([(k, y[i]) for i, k in enumerate(group)])):
                y_out = lax.dynamic_update_slice(y_out, piece, (peers[k], b, 0, 0))
        return y_out.reshape(batch_all, blk, width)

    in_specs = (act_spec, P(), P(), P(None, None, None, 'tp', None), P(None, 'tp', None, None), P(),
                P(None, None, 'tp'), P(None, 'tp'), P(None, 'tp', None), P())
    return jax.shard_map(local_fn, mesh=mesh, in_specs=in_specs, out_specs=act_spec, check_vma=False)
```

```python
import functools
import math

import jax
import jax.numpy as jnp
from jax import lax
from jax.experimental import pallas as pl
from jax.experimental.pallas import tpu as pltpu
from jax.sharding import PartitionSpec as P


LN_EPS = 1e-5
BLOCK_TOKENS = 512
TP_SIZE = 4
BLOCK_Q = 256
BLOCK_K = 256
VMEM_LIMIT = 58 * 1024 * 1024
SQRT_2_OVER_PI = math.sqrt(2.0 / math.pi)
LOG2_E = math.log2(math.e)


def layer_norm(residual, gain, bias):
    row_mean = jnp.mean(residual, axis=-1, keepdims=True)
    centered = residual - row_mean
    row_var = jnp.mean(centered * centered, axis=-1, keepdims=True)
    return (centered * lax.rsqrt(row_var + LN_EPS) * gain + bias).astype(jnp.bfloat16)


def gelu_tanh(x):
    inner = x * (SQRT_2_OVER_PI + (SQRT_2_OVER_PI * 0.044715) * (x * x))
    half = 0.5 * x
    return half + half * jnp.tanh(inner)


def dot(a, b):
    return lax.dot_general(a, b, (((1,), (0,)), ((), ())), preferred_element_type=jnp.float32)


def cost(flops, nbytes):
    return pl.CostEstimate(flops=flops, transcendentals=0, bytes_accessed=nbytes)


def start_qkv_copies(w_hbm, w_vmem, sem):
    parts, rows, _ = w_hbm.shape
    chunks = w_vmem.shape[0]
    for i in range(parts):
        half, chunk = divmod(i, chunks)
        pltpu.make_async_copy(w_hbm.at[i], w_vmem.at[chunk, pl.ds(half * rows, rows)], sem).start()


def wait_qkv_copies(w_hbm, w_vmem, sem):
    parts, rows, _ = w_hbm.shape
    chunks = w_vmem.shape[0]
    for i in range(parts):
        half, chunk = divmod(i, chunks)
        pltpu.make_async_copy(w_hbm.at[i], w_vmem.at[chunk, pl.ds(half * rows, rows)], sem).wait()


def project_qkv(h, w_vmem, qkv_ref, rows):
    for c in range(w_vmem.shape[0]):
        qkv_ref[c, rows, :] = dot(h, w_vmem[c]).astype(jnp.bfloat16)


def norm_project(x_of, splits, gain_ref, bias_ref, w_vmem, qkv_ref):
    for lo, hi in splits:
        h = layer_norm(x_of(lo, hi), gain_ref[...], bias_ref[...])
        project_qkv(h, w_vmem, qkv_ref, slice(lo, hi))


def qkv_kernel(place_ref, *refs, pieces, seq):
    piece_refs = refs[:pieces]
    own_ref, gain_ref, bias_ref, w_hbm = refs[pieces:pieces + 4]
    qkv_ref, res_ref, x_vmem, w_vmem, sems = refs[-5:]
    blk = own_ref.shape[1]
    step = pl.program_id(0)

    @pl.when(step == 0)
    def _():
        start_qkv_copies(w_hbm, w_vmem, sems.at[0])
        sources = [ref.at[0, 0] for ref in piece_refs] + [own_ref.at[place_ref[pieces] * place_ref[pieces + 1] + seq]]
        copies = [pltpu.make_async_copy(src, x_vmem.at[pl.ds(place_ref[n] * blk, blk)], sems.at[1])
                  for n, src in enumerate(sources)]
        for cp in copies:
            cp.start()
        for cp in copies:
            cp.wait()
        wait_qkv_copies(w_hbm, w_vmem, sems.at[0])

    row0 = pl.multiple_of(step * BLOCK_TOKENS, BLOCK_TOKENS)
    res_ref[...] = x_vmem[pl.ds(row0, BLOCK_TOKENS), :]
    quarter = BLOCK_TOKENS // 4
    norm_project(lambda lo, hi: x_vmem[pl.ds(row0 + lo, hi - lo), :].astype(jnp.float32),
                 ((0, quarter), (quarter, BLOCK_TOKENS)), gain_ref, bias_ref, w_vmem, qkv_ref)


def qkv_call(place, received, x_own, seq, batch, gain, bias, w_qkv, buffer):
    blk, width = x_own.shape[1:]
    tokens = blk * (len(received) + 1)
    offset = seq * tokens // BLOCK_TOKENS
    parts, rows, cols = w_qkv.shape
    chunks = parts * rows // width
    hbm = pl.BlockSpec(memory_space=pl.ANY)
    vec = pl.BlockSpec((1, width), lambda i, place: (0, 0))
    held = [] if buffer is None else [buffer]
    n_in = len(received) + 5
    return pl.pallas_call(
        functools.partial(qkv_kernel, pieces=len(received), seq=seq),
        grid_spec=pltpu.PrefetchScalarGridSpec(
            num_scalar_prefetch=1,
            grid=(tokens // BLOCK_TOKENS,),
            in_specs=[hbm] * (len(received) + 1) + [vec, vec, hbm] + [hbm for _ in held],
            out_specs=[pl.BlockSpec((chunks, BLOCK_TOKENS, cols), lambda i, place: (0, i, 0)),
                       pl.BlockSpec((BLOCK_TOKENS, width), lambda i, place: (offset + i, 0))],
            scratch_shapes=[pltpu.VMEM((tokens, width), jnp.bfloat16), pltpu.VMEM((chunks, width, cols), jnp.bfloat16),
                            pltpu.SemaphoreType.DMA((2,))]),
        out_shape=[jax.ShapeDtypeStruct((chunks, tokens, cols), jnp.bfloat16),
                   jax.ShapeDtypeStruct((batch * tokens, width), jnp.bfloat16)],
        input_output_aliases={n_in: 1} if held else {},
        compiler_params=pltpu.CompilerParams(
            dimension_semantics=('arbitrary',), vmem_limit_bytes=VMEM_LIMIT),
        cost_estimate=cost(2 * tokens * width * chunks * cols, 2 * tokens * (width + chunks * cols) + 2 * width * chunks * cols),
        name='ln_qkv',
    )(place, *received, x_own, gain, bias, w_qkv, *held)


def attention_kernel(*refs, head_dim):
    q_ref, k_ref, v_ref = refs[:3]
    o_ref, s_ref, vx_ref = refs[-3:]
    seq_len, pair = q_ref.shape[1:]
    vx_ref[:, :pair] = v_ref[0]

    @pl.when(pl.program_id(0) == 0)
    def _():
        vx_ref[:, pair:] = jnp.ones((seq_len, pair), jnp.bfloat16)

    low_lane = lax.broadcasted_iota(jnp.int32, (1, pair), 1) < head_dim
    q_pos = lax.broadcasted_iota(jnp.int32, (BLOCK_Q, BLOCK_K), 0)
    k_pos = lax.broadcasted_iota(jnp.int32, (BLOCK_Q, BLOCK_K), 1)
    causal = k_pos <= q_pos
    inv_sqrt = head_dim ** -0.5
    n_blocks = seq_len // BLOCK_Q
    order = list(range(0, n_blocks, 2)) + list(range(1, n_blocks, 2))[::-1]
    units = [(block, head) for block in order for head in range(2)]

    def head_query(unit):
        block, head = unit
        q_blk = q_ref[0, block * BLOCK_Q:(block + 1) * BLOCK_Q, :] * jnp.bfloat16(inv_sqrt)
        keep = low_lane if head == 0 else jnp.logical_not(low_lane)
        return jnp.where(keep, q_blk, jnp.zeros_like(q_blk))

    def score_chunk(unit_idx, q_h, c, run_max):
        block, _ = units[unit_idx]
        k_blk = k_ref[0, c * BLOCK_K:(c + 1) * BLOCK_K, :]
        s = lax.dot_general(q_h, k_blk, (((1,), (1,)), ((), ())), preferred_element_type=jnp.float32)
        if c == block:
            s = jnp.where(causal, s, -jnp.inf)
        s_ref[unit_idx % 2, :, c * BLOCK_K:(c + 1) * BLOCK_K] = s
        chunk_max = s[:, :128]
        for j in range(1, BLOCK_K // 128):
            chunk_max = jnp.maximum(chunk_max, s[:, j * 128:(j + 1) * 128])
        return chunk_max if run_max is None else jnp.maximum(run_max, chunk_max)

    def value_chunk(unit_idx, row_max, c):
        s = s_ref[unit_idx % 2, :, c * BLOCK_K:(c + 1) * BLOCK_K]
        p = jnp.exp2((s - row_max) * LOG2_E).astype(jnp.bfloat16)
        return dot(p, vx_ref[c * BLOCK_K:(c + 1) * BLOCK_K, :])

    run_max = None
    row_max = None
    held = None
    for step in range(len(units) + 1):
        n_score = units[step][0] + 1 if step < len(units) else 0
        n_value = units[step - 1][0] + 1 if step > 0 else 0
        if step > 0:
            row_max = jnp.max(run_max, axis=1, keepdims=True)
        run_max = None
        acc = None
        q_h = head_query(units[step]) if n_score else None
        for c in range(max(n_score, n_value)):
            if c < n_score:
                run_max = score_chunk(step, q_h, c, run_max)
            if c < n_value:
                part = value_chunk(step - 1, row_max, c)
                acc = part if acc is None else acc + part
        if n_value:
            block, head = units[step - 1]
            out = acc[:, :pair] / acc[:, pair:]
            if head == 0:
                held = out
            else:
                o_ref[block * BLOCK_Q:(block + 1) * BLOCK_Q, :] = jnp.where(low_lane, held, out).astype(jnp.bfloat16)


def attention_call(qkv, qkv_seq, seq, batch, seq_len, head_dim, buffer):
    chunks, _, cols = qkv.shape
    pair = 2 * head_dim
    subs = cols // 3 // pair
    spec = lambda t: pl.BlockSpec((1, seq_len, pair), lambda g: (g // subs, qkv_seq, t * subs + g % subs))
    held = [] if buffer is None else [buffer]
    return pl.pallas_call(
        functools.partial(attention_kernel, head_dim=head_dim),
        grid=(chunks * subs,),
        in_specs=[spec(0), spec(1), spec(2)] + [pl.BlockSpec(memory_space=pl.ANY) for _ in held],
        out_specs=pl.BlockSpec((seq_len, pair), lambda g: (seq, g)),
        out_shape=jax.ShapeDtypeStruct((batch * seq_len, chunks * subs * pair), jnp.bfloat16),
        input_output_aliases={3: 0} if held else {},
        scratch_shapes=[pltpu.VMEM((2, BLOCK_Q, seq_len), jnp.float32), pltpu.VMEM((seq_len, 2 * pair), jnp.bfloat16)],
        compiler_params=pltpu.CompilerParams(
            dimension_semantics=('arbitrary',), vmem_limit_bytes=VMEM_LIMIT),
        cost_estimate=cost(9 * seq_len * seq_len * chunks * cols // 4, 2 * seq_len * chunks * (cols + subs * pair)),
        name='causal_attention',
    )(qkv, qkv, qkv, *held)


def ffn_body(first, r_ref, o_ref, gain_ref, bias_ref, bsum_ref, bup_ref, wout_hbm, wup_hbm, wdown_hbm,
             acc_ref, wout_vmem, wup_vmem, wdown_vmem, sems, emit, more_waits=lambda: None):
    parts = wup_vmem.shape[0]
    early = 2
    out_rows = wout_hbm.shape[1]
    early_copies = []
    for i in range(parts):
        pos = (i % TP_SIZE) * (parts // TP_SIZE) + i // TP_SIZE
        early_copies.append(pltpu.make_async_copy(wout_hbm.at[i], wout_vmem.at[pl.ds(pos * out_rows, out_rows)], sems.at[0]))
    late_copies = []
    for lo, hi, sem, group in ((0, early, 0, early_copies), (early, parts, 1, late_copies)):
        for src, dst in ((wup_hbm, wup_vmem), (wdown_hbm, wdown_vmem)):
            group.append(pltpu.make_async_copy(src.at[pl.ds(lo, hi - lo)], dst.at[pl.ds(lo, hi - lo)], sems.at[sem]))

    @pl.when(first)
    def _():
        for cp in early_copies + late_copies:
            cp.start()
        for cp in early_copies:
            cp.wait()

    acc_ref[...] = dot(o_ref[...], wout_vmem[...]) + bsum_ref[...]
    h = layer_norm(r_ref[...].astype(jnp.float32), gain_ref[...], bias_ref[...])
    hidden = dot(h, wup_vmem[0]) + bup_ref[0]
    half = BLOCK_TOKENS // 2
    for c in range(parts):
        if c + 1 == early:
            @pl.when(first)
            def _():
                for cp in late_copies:
                    cp.wait()
                more_waits()
        ahead = dot(h, wup_vmem[c + 1]) + bup_ref[c + 1] if c + 1 < parts else None
        gelu_out = gelu_tanh(hidden).astype(jnp.bfloat16)
        if c + 1 < parts:
            acc_ref[...] += dot(gelu_out, wdown_vmem[c])
        else:
            for rows in (slice(0, half), slice(half, BLOCK_TOKENS)):
                emit(rows, r_ref[rows, :].astype(jnp.float32) + (acc_ref[rows, :] + dot(gelu_out[rows, :], wdown_vmem[c])))
        hidden = ahead


def mid_kernel(r_ref, o_ref, gain_ref, bias_ref, bsum_ref, bup_ref, ngain_ref, nbias_ref, wout_hbm, wup_hbm, wdown_hbm,
               wqkv_hbm, res_ref, qkv_ref, acc_ref, wout_vmem, wup_vmem, wdown_vmem, wqkv_vmem, sems):
    first = pl.program_id(0) == 0

    @pl.when(first)
    def _():
        start_qkv_copies(wqkv_hbm, wqkv_vmem, sems.at[2])

    rows_done = []

    def emit(rows, r_new):
        res_ref[rows, :] = r_new
        rows_done.append((rows, r_new))

    ffn_body(first, r_ref, o_ref, gain_ref, bias_ref, bsum_ref, bup_ref, wout_hbm, wup_hbm, wdown_hbm,
             acc_ref, wout_vmem, wup_vmem, wdown_vmem, sems, emit,
             lambda: wait_qkv_copies(wqkv_hbm, wqkv_vmem, sems.at[2]))
    for rows, r_new in rows_done:
        project_qkv(layer_norm(r_new, ngain_ref[...], nbias_ref[...]), wqkv_vmem, qkv_ref, rows)


def last_kernel(rows_ref, r_ref, o_ref, gain_ref, bias_ref, bsum_ref, bup_ref, wout_hbm, wup_hbm, wdown_hbm,
                y_ref, acc_ref, wout_vmem, wup_vmem, wdown_vmem, sems):
    first = pl.program_id(0) == 0

    def emit(rows, r_new):
        y_ref[rows, :] = r_new.astype(jnp.bfloat16)

    ffn_body(first, r_ref, o_ref, gain_ref, bias_ref, bsum_ref, bup_ref, wout_hbm, wup_hbm, wdown_hbm,
             acc_ref, wout_vmem, wup_vmem, wdown_vmem, sems, emit)


def mid_call(r, o, gain, bias, bsum, bup, ngain, nbias, w_out, w_up, w_down, w_qkv):
    tokens, width = r.shape
    parts, rows, cols = w_qkv.shape
    chunks = parts * rows // width
    row = pl.BlockSpec((BLOCK_TOKENS, width), lambda i: (i, 0))
    vec = pl.BlockSpec((1, width), lambda i: (0, 0))
    bup_spec = pl.BlockSpec(bup.shape, lambda i: (0, 0, 0))
    hbm = pl.BlockSpec(memory_space=pl.ANY)
    return pl.pallas_call(
        mid_kernel,
        grid=(tokens // BLOCK_TOKENS,),
        in_specs=[row, row, vec, vec, vec, bup_spec, vec, vec, hbm, hbm, hbm, hbm],
        out_specs=[row, pl.BlockSpec((chunks, BLOCK_TOKENS, cols), lambda i: (0, i, 0))],
        out_shape=[jax.ShapeDtypeStruct((tokens, width), jnp.float32),
                   jax.ShapeDtypeStruct((chunks, tokens, cols), jnp.bfloat16)],
        scratch_shapes=[pltpu.VMEM((BLOCK_TOKENS, width), jnp.float32), pltpu.VMEM((width, width), jnp.bfloat16),
                        pltpu.VMEM(w_up.shape, jnp.bfloat16), pltpu.VMEM(w_down.shape, jnp.bfloat16),
                        pltpu.VMEM((chunks, width, cols), jnp.bfloat16), pltpu.SemaphoreType.DMA((3,))],
        compiler_params=pltpu.CompilerParams(
            dimension_semantics=('arbitrary',), vmem_limit_bytes=VMEM_LIMIT),
        cost_estimate=cost(24 * tokens * width * width, 20 * tokens * width),
        name='ffn_qkv',
    )(r, o, gain, bias, bsum, bup, ngain, nbias, w_out, w_up, w_down, w_qkv)


def last_call(r, o, gain, bias, bsum, bup, w_out, w_up, w_down, blocks, blk):
    width = r.shape[1]
    count = blocks.shape[0] * blk
    per = blk // BLOCK_TOKENS
    row = pl.BlockSpec((BLOCK_TOKENS, width), lambda i, rows: (rows[i // per] * per + i % per, 0))
    vec = pl.BlockSpec((1, width), lambda i, rows: (0, 0))
    hbm = pl.BlockSpec(memory_space=pl.ANY)
    return pl.pallas_call(
        last_kernel,
        grid_spec=pltpu.PrefetchScalarGridSpec(
            num_scalar_prefetch=1,
            grid=(count // BLOCK_TOKENS,),
            in_specs=[row, row,
                      vec, vec, vec, pl.BlockSpec(bup.shape, lambda i, rows: (0, 0, 0)), hbm, hbm, hbm],
            out_specs=pl.BlockSpec((BLOCK_TOKENS, width), lambda i, rows: (i, 0)),
            scratch_shapes=[pltpu.VMEM((BLOCK_TOKENS, width), jnp.float32), pltpu.VMEM((width, width), jnp.bfloat16),
                            pltpu.VMEM(w_up.shape, jnp.bfloat16), pltpu.VMEM(w_down.shape, jnp.bfloat16),
                            pltpu.SemaphoreType.DMA((2,))]),
        out_shape=jax.ShapeDtypeStruct((count, width), jnp.bfloat16),
        compiler_params=pltpu.CompilerParams(
            dimension_semantics=('arbitrary',), vmem_limit_bytes=VMEM_LIMIT),
        cost_estimate=cost(18 * count * width * width, 8 * count * width),
        name='ffn_out',
    )(blocks, r, o, gain, bias, bsum, bup, w_out, w_up, w_down)


def solution(mesh):
    tp_size = mesh.shape['tp']
    dp_size = mesh.shape['dp']
    act_spec = P('dp', 'tp', None)

    def local_fn(x_in, ln_gain, ln_bias, w_qkv, w_out, b_out, w_up, b_up, w_down, b_down):
        n_layers, width, _, heads, head_dim = w_qkv.shape
        ffn = w_up.shape[2]
        dp_idx = lax.axis_index('dp')
        tp_idx = lax.axis_index('tp')
        batch_all, blk, _ = x_in.shape
        batch = batch_all // tp_size
        seq_len = blk * tp_size

        def gather(shard):
            return lax.all_gather(shard, ('dp', 'tp'), axis=0, tiled=False)

        def half(arr, layer, axis):
            sizes = [1, *arr.shape[1:]]
            sizes[axis] //= dp_size
            start = [layer] + [0] * (arr.ndim - 1)
            start[axis] = dp_idx * sizes[axis]
            return lax.dynamic_slice(arr, start, sizes)[0]

        def qkv_shard(layer, w_qkv):
            return half(w_qkv, layer, 1).reshape(width // dp_size, 3 * heads * head_dim)

        def ffn_shards(layer, w_out, w_up, w_down):
            return (half(w_out, layer, 1).reshape(heads * head_dim // dp_size, width), half(w_up, layer, 2),
                    half(w_down, layer, 1))

        def exchange(pieces):
            return [piece if k == 0 else lax.ppermute(piece, 'tp', [(i, i ^ k) for i in range(tp_size)])
                    for k, piece in pieces]

        def ffn_weights(shards):
            return tuple(gather(shard) for shard in shards)

        bsum = b_out + b_down
        peers = [jnp.bitwise_xor(tp_idx, k) for k in range(tp_size)]
        far_first = [k for k in reversed(range(tp_size))]

        x_parts = x_in.reshape(tp_size, batch, blk, width)
        place = jnp.stack([peers[k] for k in far_first] + [jnp.full_like(tp_idx, batch)]).astype(jnp.int32)

        def x_send(parts, b):
            return [(k, lax.dynamic_slice(parts, (peers[k], b, 0, 0), (1, 1, blk, width))) for k in far_first if k]

        first_shard = qkv_shard(0, w_qkv)
        qkv_w = gather(first_shard)
        received = exchange(x_send(x_parts, 0))
        biases = exchange([(k, b_up) for k in range(tp_size)])
        bup_all = jnp.zeros((tp_size, n_layers, ffn), jnp.float32)
        for k, piece in enumerate(biases):
            bup_all = lax.dynamic_update_slice(bup_all, piece[None], (peers[k], 0, 0))
        bup_all = bup_all.reshape(tp_size, n_layers, dp_size, ffn // dp_size).transpose(1, 2, 0, 3)
        bup_all = bup_all.reshape(n_layers, dp_size * tp_size, 1, ffn // dp_size)
        first_shard, received, bup_all = lax.optimization_barrier((first_shard, received, bup_all))
        received, x_later, shards = lax.optimization_barrier((received, x_parts, ffn_shards(0, w_out, w_up, w_down)))
        pieces = [received] + [exchange(x_send(x_later, b)) for b in range(1, batch)]
        weights = [ffn_weights(shards)]

        def norm_args(layer):
            return ln_gain[layer:layer + 1], ln_bias[layer:layer + 1]

        qkv, residual, attn = None, None, None
        params = (w_qkv, w_out, w_up, w_down)
        for b in range(batch):
            got = pieces[b]
            if b:
                got, attn, params = lax.optimization_barrier((got, attn, params))
            qkv, residual = qkv_call(place, got, x_in, b, batch, *norm_args(0), qkv_w, residual)
            attn = attention_call(qkv, 0, b, batch, seq_len, head_dim, attn)
        later_qkv = []
        for layer in range(1, n_layers):
            later_qkv.append(gather(qkv_shard(layer, params[0])))
            weights.append(ffn_weights(ffn_shards(layer, *params[1:])))

        def args(layer):
            return (*norm_args(layer), bsum[layer:layer + 1], bup_all[layer])

        for layer in range(n_layers - 1):
            if layer:
                attn = None
                for b in range(batch):
                    attn = attention_call(qkv_all, b, b, batch, seq_len, head_dim, attn)
            residual, qkv_all = mid_call(residual, attn, *args(layer), *norm_args(layer + 1), *weights[layer],
                                         later_qkv[layer])
        layer = n_layers - 1
        far, near = far_first[:tp_size // 2], far_first[tp_size // 2:]
        attn, done, sent = None, None, []

        def finish(todo):
            order = jnp.stack([b * tp_size + peers[k] for b, k in todo]).astype(jnp.int32)
            if done is not None:
                order, sent[-1] = lax.optimization_barrier((order, done))
            y = last_call(residual, attn, *args(layer), *weights[layer], order, blk)
            todos.append(todo)
            sent.append(y)
            return y

        todos = []
        for b in range(batch):
            if done is not None:
                qkv_all, sent[-1] = lax.optimization_barrier((qkv_all, done))
                done = sent[-1]
            attn = attention_call(qkv_all, b, b, batch, seq_len, head_dim, attn)
            done = finish([(b, k) for k in far])
        finish([(b, k) for b in range(batch) for k in near])
        y_out = jnp.zeros((tp_size, batch, blk, width), jnp.bfloat16)
        for todo, y in zip(todos, sent):
            y = y.reshape(len(todo), 1, 1, blk, width)
            got = exchange([(k, y[i]) for i, (_, k) in enumerate(todo)])
            for (b, k), piece in zip(todo, got):
                y_out = lax.dynamic_update_slice(y_out, piece, (peers[k], b, 0, 0))
        return y_out.reshape(batch_all, blk, width)

    in_specs = (act_spec, P(), P(), P(None, None, None, 'tp', None), P(None, 'tp', None, None), P(),
                P(None, None, 'tp'), P(None, 'tp'), P(None, 'tp', None), P())
    return jax.shard_map(local_fn, mesh=mesh, in_specs=in_specs, out_specs=act_spec, check_vma=False)
```

```python
import functools
import math

import jax
import jax.numpy as jnp
from jax import lax
from jax.experimental import pallas as pl
from jax.experimental.layout import Layout, with_layout_constraint
from jax.experimental.pallas import tpu as pltpu
from jax.sharding import PartitionSpec as P


LN_EPS = 1e-5
BLOCK_TOKENS = 512
TP_SIZE = 4
BLOCK_Q = 256
BLOCK_K = 256
VMEM_LIMIT = 58 * 1024 * 1024
SQRT_2_OVER_PI = math.sqrt(2.0 / math.pi)
LOG2_E = math.log2(math.e)


def layer_norm(residual, gain, bias):
    row_mean = jnp.mean(residual, axis=-1, keepdims=True)
    centered = residual - row_mean
    row_var = jnp.mean(centered * centered, axis=-1, keepdims=True)
    return (centered * lax.rsqrt(row_var + LN_EPS) * gain + bias).astype(jnp.bfloat16)


def gelu_tanh(x):
    inner = x * (SQRT_2_OVER_PI + (SQRT_2_OVER_PI * 0.044715) * (x * x))
    half = 0.5 * x
    return half + half * jnp.tanh(inner)


def dot(a, b):
    return lax.dot_general(a, b, (((1,), (0,)), ((), ())), preferred_element_type=jnp.float32)


def cost(flops, nbytes):
    return pl.CostEstimate(flops=flops, transcendentals=0, bytes_accessed=nbytes)


def start_qkv_copies(w_hbm, w_vmem, sem):
    parts, rows, _ = w_hbm.shape
    chunks = w_vmem.shape[0]
    for i in range(parts):
        half, chunk = divmod(i, chunks)
        pltpu.make_async_copy(w_hbm.at[i], w_vmem.at[chunk, pl.ds(half * rows, rows)], sem).start()


def wait_qkv_copies(w_hbm, w_vmem, sem):
    parts, rows, _ = w_hbm.shape
    chunks = w_vmem.shape[0]
    for i in range(parts):
        half, chunk = divmod(i, chunks)
        pltpu.make_async_copy(w_hbm.at[i], w_vmem.at[chunk, pl.ds(half * rows, rows)], sem).wait()


def project_qkv(h, w_vmem, qkv_ref):
    for c in range(w_vmem.shape[0]):
        qkv_ref[c] = dot(h, w_vmem[c]).astype(jnp.bfloat16)


def next_qkv_kernel(r_ref, gain_ref, bias_ref, w_hbm, qkv_ref, w_vmem, sem):
    @pl.when(pl.program_id(0) == 0)
    def _():
        start_qkv_copies(w_hbm, w_vmem, sem)
        wait_qkv_copies(w_hbm, w_vmem, sem)

    project_qkv(layer_norm(r_ref[...], gain_ref[...], bias_ref[...]), w_vmem, qkv_ref)


def next_qkv_call(r, gain, bias, w_qkv):
    tokens, width = r.shape
    parts, rows, cols = w_qkv.shape
    chunks = parts * rows // width
    vec = pl.BlockSpec((1, width), lambda i: (0, 0))
    return pl.pallas_call(
        next_qkv_kernel,
        grid=(tokens // BLOCK_TOKENS,),
        in_specs=[pl.BlockSpec((BLOCK_TOKENS, width), lambda i: (i, 0)), vec, vec, pl.BlockSpec(memory_space=pl.ANY)],
        out_specs=pl.BlockSpec((chunks, BLOCK_TOKENS, cols), lambda i: (0, i, 0)),
        out_shape=jax.ShapeDtypeStruct((chunks, tokens, cols), jnp.bfloat16),
        scratch_shapes=[pltpu.VMEM((chunks, width, cols), jnp.bfloat16), pltpu.SemaphoreType.DMA],
        compiler_params=pltpu.CompilerParams(
            dimension_semantics=('arbitrary',), vmem_limit_bytes=VMEM_LIMIT),
        cost_estimate=cost(2 * tokens * width * chunks * cols, 2 * tokens * (2 * width + chunks * cols)),
        name='next_qkv',
    )(r, gain, bias, w_qkv)


def qkv_kernel(place_ref, *refs, pieces, seq):
    piece_refs = refs[:pieces]
    own_ref, gain_ref, bias_ref, w_hbm = refs[pieces:pieces + 4]
    qkv_ref, res_ref, x_vmem, w_vmem, sems = refs[-5:]
    blk = own_ref.shape[1]
    step = pl.program_id(0)

    @pl.when(step == 0)
    def _():
        start_qkv_copies(w_hbm, w_vmem, sems.at[0])
        sources = [ref.at[0, 0] for ref in piece_refs] + [own_ref.at[place_ref[pieces] * place_ref[pieces + 1] + seq]]
        copies = [pltpu.make_async_copy(src, x_vmem.at[pl.ds(place_ref[n] * blk, blk)], sems.at[1])
                  for n, src in enumerate(sources)]
        for cp in copies:
            cp.start()
        for cp in copies:
            cp.wait()
        wait_qkv_copies(w_hbm, w_vmem, sems.at[0])

    row0 = pl.multiple_of(step * BLOCK_TOKENS, BLOCK_TOKENS)
    res_ref[...] = x_vmem[pl.ds(row0, BLOCK_TOKENS), :]
    h = layer_norm(x_vmem[pl.ds(row0, BLOCK_TOKENS), :].astype(jnp.float32), gain_ref[...], bias_ref[...])
    project_qkv(h, w_vmem, qkv_ref)


def qkv_call(place, received, x_own, seq, batch, gain, bias, w_qkv, buffer):
    blk, width = x_own.shape[1:]
    tokens = blk * (len(received) + 1)
    offset = seq * tokens // BLOCK_TOKENS
    parts, rows, cols = w_qkv.shape
    chunks = parts * rows // width
    hbm = pl.BlockSpec(memory_space=pl.ANY)
    vec = pl.BlockSpec((1, width), lambda i, place: (0, 0))
    held = [] if buffer is None else [buffer]
    n_in = len(received) + 5
    return pl.pallas_call(
        functools.partial(qkv_kernel, pieces=len(received), seq=seq),
        grid_spec=pltpu.PrefetchScalarGridSpec(
            num_scalar_prefetch=1,
            grid=(tokens // BLOCK_TOKENS,),
            in_specs=[hbm] * (len(received) + 1) + [vec, vec, hbm] + [hbm for _ in held],
            out_specs=[pl.BlockSpec((chunks, BLOCK_TOKENS, cols), lambda i, place: (0, i, 0)),
                       pl.BlockSpec((BLOCK_TOKENS, width), lambda i, place: (offset + i, 0))],
            scratch_shapes=[pltpu.VMEM((tokens, width), jnp.bfloat16), pltpu.VMEM((chunks, width, cols), jnp.bfloat16),
                            pltpu.SemaphoreType.DMA((2,))]),
        out_shape=[jax.ShapeDtypeStruct((chunks, tokens, cols), jnp.bfloat16),
                   jax.ShapeDtypeStruct((batch * tokens, width), jnp.bfloat16)],
        input_output_aliases={n_in: 1} if held else {},
        compiler_params=pltpu.CompilerParams(
            dimension_semantics=('arbitrary',), vmem_limit_bytes=VMEM_LIMIT),
        cost_estimate=cost(2 * tokens * width * chunks * cols, 2 * tokens * (width + chunks * cols) + 2 * width * chunks * cols),
        name='ln_qkv',
    )(place, *received, x_own, gain, bias, w_qkv, *held)


def attention_kernel(*refs, head_dim):
    q_ref, k_ref, v_ref = refs[:3]
    o_ref, s_ref, vx_ref = refs[-3:]
    seq_len, pair = q_ref.shape[1:]
    vx_ref[:, :pair] = v_ref[0]

    @pl.when(pl.program_id(0) == 0)
    def _():
        vx_ref[:, pair:] = jnp.ones((seq_len, pair), jnp.bfloat16)

    low_lane = lax.broadcasted_iota(jnp.int32, (1, pair), 1) < head_dim
    rows = 2 * BLOCK_Q
    q_pos = lax.broadcasted_iota(jnp.int32, (rows, BLOCK_K), 0) % BLOCK_Q
    k_pos = lax.broadcasted_iota(jnp.int32, (rows, BLOCK_K), 1)
    causal = k_pos <= q_pos
    inv_sqrt = head_dim ** -0.5
    n_blocks = seq_len // BLOCK_Q
    units = list(range(0, n_blocks, 2)) + list(range(1, n_blocks, 2))[::-1]

    def stacked_query(block):
        q_blk = q_ref[0, block * BLOCK_Q:(block + 1) * BLOCK_Q, :] * jnp.bfloat16(inv_sqrt)
        zero = jnp.zeros_like(q_blk)
        return jnp.concatenate([jnp.where(low_lane, q_blk, zero), jnp.where(low_lane, zero, q_blk)], axis=0)

    def score_chunk(slot, block, q_h, c, run_max):
        k_blk = k_ref[0, c * BLOCK_K:(c + 1) * BLOCK_K, :]
        s = lax.dot_general(q_h, k_blk, (((1,), (1,)), ((), ())), preferred_element_type=jnp.float32)
        if c == block:
            s = jnp.where(causal, s, -jnp.inf)
        s_ref[slot, :, c * BLOCK_K:(c + 1) * BLOCK_K] = s
        chunk_max = s[:, :128]
        for j in range(1, BLOCK_K // 128):
            chunk_max = jnp.maximum(chunk_max, s[:, j * 128:(j + 1) * 128])
        return chunk_max if run_max is None else jnp.maximum(run_max, chunk_max)

    def value_chunk(slot, row_max, c):
        s = s_ref[slot, :, c * BLOCK_K:(c + 1) * BLOCK_K]
        p = jnp.exp2((s - row_max) * LOG2_E).astype(jnp.bfloat16)
        return dot(p, vx_ref[c * BLOCK_K:(c + 1) * BLOCK_K, :])

    run_max = None
    for step in range(len(units) + 1):
        n_score = units[step] + 1 if step < len(units) else 0
        n_value = units[step - 1] + 1 if step > 0 else 0
        row_max = jnp.max(run_max, axis=1, keepdims=True) if step > 0 else None
        run_max = None
        acc = None
        q_h = stacked_query(units[step]) if n_score else None
        for c in range(max(n_score, n_value)):
            if c < n_score:
                run_max = score_chunk(step % 2, units[step], q_h, c, run_max)
            if c < n_value:
                part = value_chunk((step - 1) % 2, row_max, c)
                acc = part if acc is None else acc + part
        if n_value:
            block = units[step - 1]
            out = acc[:, :pair] / acc[:, pair:]
            o_ref[block * BLOCK_Q:(block + 1) * BLOCK_Q, :] = jnp.where(low_lane, out[:BLOCK_Q], out[BLOCK_Q:]).astype(jnp.bfloat16)


def attention_call(qkv, qkv_seq, seq, batch, seq_len, head_dim, buffer):
    chunks, _, cols = qkv.shape
    pair = 2 * head_dim
    subs = cols // 3 // pair
    spec = lambda t: pl.BlockSpec((1, seq_len, pair), lambda g: (g // subs, qkv_seq, t * subs + g % subs))
    held = [] if buffer is None else [buffer]
    return pl.pallas_call(
        functools.partial(attention_kernel, head_dim=head_dim),
        grid=(chunks * subs,),
        in_specs=[spec(0), spec(1), spec(2)] + [pl.BlockSpec(memory_space=pl.ANY) for _ in held],
        out_specs=pl.BlockSpec((seq_len, pair), lambda g: (seq, g)),
        out_shape=jax.ShapeDtypeStruct((batch * seq_len, chunks * subs * pair), jnp.bfloat16),
        input_output_aliases={3: 0} if held else {},
        scratch_shapes=[pltpu.VMEM((2, 2 * BLOCK_Q, seq_len), jnp.float32), pltpu.VMEM((seq_len, 2 * pair), jnp.bfloat16)],
        compiler_params=pltpu.CompilerParams(
            dimension_semantics=('arbitrary',), vmem_limit_bytes=VMEM_LIMIT),
        cost_estimate=cost(9 * seq_len * seq_len * chunks * cols // 4, 2 * seq_len * chunks * (cols + subs * pair)),
        name='causal_attention',
    )(qkv, qkv, qkv, *held)


def ffn_body(first, r_ref, o_ref, gain_ref, bias_ref, bsum_ref, bup_ref, wout_hbm, wup_hbm, wdown_hbm,
             acc_ref, wout_vmem, wup_vmem, wdown_vmem, sems, emit):
    parts = wup_vmem.shape[0]
    early = 2
    out_rows = wout_hbm.shape[1]
    early_copies = []
    for i in range(parts):
        pos = (i % TP_SIZE) * (parts // TP_SIZE) + i // TP_SIZE
        early_copies.append(pltpu.make_async_copy(wout_hbm.at[i], wout_vmem.at[pl.ds(pos * out_rows, out_rows)], sems.at[0]))
    late_copies = []
    for lo, hi, sem, group in ((0, early, 0, early_copies), (early, parts, 1, late_copies)):
        for src, dst in ((wup_hbm, wup_vmem), (wdown_hbm, wdown_vmem)):
            group.append(pltpu.make_async_copy(src.at[pl.ds(lo, hi - lo)], dst.at[pl.ds(lo, hi - lo)], sems.at[sem]))

    @pl.when(first)
    def _():
        for cp in early_copies + late_copies:
            cp.start()
        for cp in early_copies:
            cp.wait()

    acc_ref[...] = dot(o_ref[...], wout_vmem[...]) + bsum_ref[...]
    h = layer_norm(r_ref[...].astype(jnp.float32), gain_ref[...], bias_ref[...])
    hidden = dot(h, wup_vmem[0]) + bup_ref[0]
    half = BLOCK_TOKENS // 2
    for c in range(parts):
        if c + 1 == early:
            @pl.when(first)
            def _():
                for cp in late_copies:
                    cp.wait()
        ahead = dot(h, wup_vmem[c + 1]) + bup_ref[c + 1] if c + 1 < parts else None
        gelu_out = gelu_tanh(hidden).astype(jnp.bfloat16)
        if c + 1 < parts:
            acc_ref[...] += dot(gelu_out, wdown_vmem[c])
        else:
            for rows in (slice(0, half), slice(half, BLOCK_TOKENS)):
                emit(rows, r_ref[rows, :].astype(jnp.float32) + (acc_ref[rows, :] + dot(gelu_out[rows, :], wdown_vmem[c])))
        hidden = ahead


def block_kernel(rows_ref, r_ref, o_ref, gain_ref, bias_ref, bsum_ref, bup_ref, wout_hbm, wup_hbm, wdown_hbm,
                y_ref, acc_ref, wout_vmem, wup_vmem, wdown_vmem, sems):
    first = pl.program_id(0) == 0

    def emit(rows, r_new):
        y_ref[rows, :] = r_new.astype(y_ref.dtype)

    ffn_body(first, r_ref, o_ref, gain_ref, bias_ref, bsum_ref, bup_ref, wout_hbm, wup_hbm, wdown_hbm,
             acc_ref, wout_vmem, wup_vmem, wdown_vmem, sems, emit)


def block_call(r, o, gain, bias, bsum, bup, w_out, w_up, w_down, blocks, blk, dtype):
    width = r.shape[1]
    count = blocks.shape[0] * blk
    per = blk // BLOCK_TOKENS
    row = pl.BlockSpec((BLOCK_TOKENS, width), lambda i, rows: (rows[i // per] * per + i % per, 0))
    vec = pl.BlockSpec((1, width), lambda i, rows: (0, 0))
    hbm = pl.BlockSpec(memory_space=pl.ANY)
    return pl.pallas_call(
        block_kernel,
        grid_spec=pltpu.PrefetchScalarGridSpec(
            num_scalar_prefetch=1,
            grid=(count // BLOCK_TOKENS,),
            in_specs=[row, row,
                      vec, vec, vec, pl.BlockSpec(bup.shape, lambda i, rows: (0, 0, 0)), hbm, hbm, hbm],
            out_specs=pl.BlockSpec((BLOCK_TOKENS, width), lambda i, rows: (i, 0)),
            scratch_shapes=[pltpu.VMEM((BLOCK_TOKENS, width), jnp.float32), pltpu.VMEM((width, width), jnp.bfloat16),
                            pltpu.VMEM(w_up.shape, jnp.bfloat16), pltpu.VMEM(w_down.shape, jnp.bfloat16),
                            pltpu.SemaphoreType.DMA((2,))]),
        out_shape=jax.ShapeDtypeStruct((count, width), dtype),
        compiler_params=pltpu.CompilerParams(
            dimension_semantics=('arbitrary',), vmem_limit_bytes=VMEM_LIMIT),
        cost_estimate=cost(18 * count * width * width, 8 * count * width),
        name='ffn',
    )(blocks, r, o, gain, bias, bsum, bup, w_out, w_up, w_down)


def solution(mesh):
    tp_size = mesh.shape['tp']
    dp_size = mesh.shape['dp']
    act_spec = P('dp', 'tp', None)

    def local_fn(x_in, ln_gain, ln_bias, w_qkv, w_out, b_out, w_up, b_up, w_down, b_down):
        n_layers, width, _, heads, head_dim = w_qkv.shape
        ffn = w_up.shape[2]
        dp_idx = lax.axis_index('dp')
        tp_idx = lax.axis_index('tp')
        batch_all, blk, _ = x_in.shape
        batch = batch_all // tp_size
        seq_len = blk * tp_size

        def gather(shard):
            return lax.all_gather(shard, ('dp', 'tp'), axis=0, tiled=False)

        def half(arr, layer, axis):
            sizes = [1, *arr.shape[1:]]
            sizes[axis] //= dp_size
            start = [layer] + [0] * (arr.ndim - 1)
            start[axis] = dp_idx * sizes[axis]
            return lax.dynamic_slice(arr, start, sizes)[0]

        def qkv_shard(layer, w_qkv):
            return half(w_qkv, layer, 1).reshape(width // dp_size, 3 * heads * head_dim)

        def ffn_shards(layer, w_out, w_up, w_down):
            return (half(w_out, layer, 1).reshape(heads * head_dim // dp_size, width), half(w_up, layer, 2),
                    half(w_down, layer, 1))

        def exchange(pieces):
            return [piece if k == 0 else lax.ppermute(piece, 'tp', [(i, i ^ k) for i in range(tp_size)])
                    for k, piece in pieces]

        def ffn_weights(shards):
            return tuple(gather(shard) for shard in shards)

        bsum = b_out + b_down
        peers = [jnp.bitwise_xor(tp_idx, k) for k in range(tp_size)]
        far_first = [k for k in reversed(range(tp_size))]

        x_parts = x_in.reshape(tp_size, batch, blk, width)
        place = jnp.stack([peers[k] for k in far_first] + [jnp.full_like(tp_idx, batch)]).astype(jnp.int32)

        links = [k for k in far_first if k]
        first_shard = qkv_shard(0, w_qkv)
        later_parts, _ = lax.optimization_barrier((x_parts, first_shard))
        x_send = [[lax.dynamic_slice(later_parts if b else x_parts, (peers[k], b, 0, 0), (1, 1, blk, width)) for k in links]
                  for b in range(batch)]
        qkv_w = gather(first_shard)
        received = exchange(zip(links, x_send[0]))
        biases = exchange([(k, b_up) for k in range(tp_size)])
        bup_all = jnp.zeros((tp_size, n_layers, ffn), jnp.float32)
        for k, piece in enumerate(biases):
            bup_all = lax.dynamic_update_slice(bup_all, piece[None], (peers[k], 0, 0))
        bup_all = bup_all.reshape(tp_size, n_layers, dp_size, ffn // dp_size).transpose(1, 2, 0, 3)
        bup_all = bup_all.reshape(n_layers, dp_size * tp_size, 1, ffn // dp_size)
        small = [(ln_gain[layer:layer + 1], ln_bias[layer:layer + 1], bsum[layer:layer + 1], bup_all[layer])
                 for layer in range(n_layers)]

        far, near = far_first[:tp_size // 2], far_first[tp_size // 2:]
        todos = [[(b, k) for k in far] for b in range(batch)] + [[(b, k) for b in range(batch) for k in near]]
        orders = [jnp.stack([b * tp_size + peers[k] for b, k in todo]).astype(jnp.int32) for todo in todos]

        shards = [ffn_shards(layer, w_out, w_up, w_down) for layer in range(n_layers)]
        qkv_shards = [with_layout_constraint(qkv_shard(layer, w_qkv), Layout(major_to_minor=(0, 1)))
                      for layer in range(1, n_layers)]
        received, small, orders, place, shards, qkv_shards, x_send[1:] = lax.optimization_barrier(
            (received, small, orders, place, shards, qkv_shards, x_send[1:]))
        pieces = [received] + [exchange(zip(links, x_send[b])) for b in range(1, batch)]
        weights = [ffn_weights(shards[0])]

        def norm_args(layer):
            return small[layer][:2]

        qkv, residual, attn = None, None, None
        for b in range(batch):
            got = pieces[b]
            if b:
                got, attn, shards, qkv_shards = lax.optimization_barrier((got, attn, shards, qkv_shards))
            qkv, residual = qkv_call(place, got, x_in, b, batch, *norm_args(0), qkv_w, residual)
            attn = attention_call(qkv, 0, b, batch, seq_len, head_dim, attn)
        later_qkv = []
        for layer in range(1, n_layers):
            later_qkv.append(gather(qkv_shards[layer - 1]))
            weights.append(ffn_weights(shards[layer]))

        for layer in range(n_layers - 1):
            if layer:
                attn = None
                for b in range(batch):
                    attn = attention_call(qkv_all, b, b, batch, seq_len, head_dim, attn)
            everything = jnp.arange(batch * tp_size, dtype=jnp.int32)
            residual = block_call(residual, attn, *small[layer], *weights[layer], everything, blk, jnp.float32)
            qkv_all = next_qkv_call(residual, *norm_args(layer + 1), later_qkv[layer])
        layer = n_layers - 1
        attn, done, sent = None, None, []

        def finish(order):
            if done is not None:
                order, sent[-1] = lax.optimization_barrier((order, done))
            y = block_call(residual, attn, *small[layer], *weights[layer], order, blk, jnp.bfloat16)
            sent.append(y)
            return y

        for b in range(batch):
            if done is not None:
                qkv_all, sent[-1] = lax.optimization_barrier((qkv_all, done))
                done = sent[-1]
            attn = attention_call(qkv_all, b, b, batch, seq_len, head_dim, attn)
            done = finish(orders[b])
        finish(orders[batch])
        y_out = jnp.zeros((tp_size, batch, blk, width), jnp.bfloat16)
        for todo, y in zip(todos, sent):
            y = y.reshape(len(todo), 1, 1, blk, width)
            got = exchange([(k, y[i]) for i, (_, k) in enumerate(todo)])
            for (b, k), piece in zip(todo, got):
                y_out = lax.dynamic_update_slice(y_out, piece, (peers[k], b, 0, 0))
        return y_out.reshape(batch_all, blk, width)

    in_specs = (act_spec, P(), P(), P(None, None, None, 'tp', None), P(None, 'tp', None, None), P(),
                P(None, None, 'tp'), P(None, 'tp'), P(None, 'tp', None), P())
    return jax.shard_map(local_fn, mesh=mesh, in_specs=in_specs, out_specs=act_spec, check_vma=False)
```
